32 devices in a mesh: ep: 8 (over z, y), dp: 4 (over x, core).
Axes of the slice: x: 2, y: 2, z: 4, core: 2. Of those that a mesh axis runs over, the one named last changes fastest.
Arguments:
- row_inputs: bfloat16 [4, 1024, 2048], P('dp', 'ep'), may hold values from -6 to 6
- hidden_grad: bfloat16 [4, 1024, 384], P('dp', 'ep'), may hold values from -6 to 6
- router_weight: bfloat16 [4, 1024], P('dp', 'ep'), may hold values from 0.049804688 to 1
- row_counts: int32 [4, 8, 2], P('dp', 'ep'), may hold values from 0 to 128, as said below
- row_owner: int32 [4, 1024, 1], P('dp', 'ep'), may hold values from 0 to 7; in each aligned block of 128 rows (0 to 127, 128 to 255, ..., all dimensions but the last counted through in order) at most 24 rows name the same one
- row_position: int32 [4, 1024], P('dp', 'ep'), may hold values from 0 to 127
- replica_expert: int32 [8], replicated, may hold values from 0 to 7, each once
- gate_up: bfloat16 [8, 2048, 768], P('ep', 'dp'), may hold values from -0.125 to 0.125
Outputs:
- token_grad: bfloat16 [4, 1024, 2048], P('dp', 'ep')
- weight_grad: float32 [8, 2048, 768], P('ep', 'dp')
The draws below stay inside these ranges and needn't reach their ends.
Inputs may be any that keep to these rules, and one draw needn't show every extreme that they name: `row_counts`: for each data index and ep index: live rows of the home slot, then of the replica slot; together at most 128, and exactly 128 on some device of every data index. `row_owner`: within the rows of one device at most 24 rows name the same owner; some device has exactly 24 rows naming one owner. `replica_expert`: A permutation: every expert has exactly one replica slot.
All inputs are finite; a program needn't handle non-finite values.
Results may differ from the reference program's by a relative error of at most 0.012.
Values may be sent and summed in bfloat16 or wider, within the bound.
No kernel may reach another device: no remote copies, remote signals or barrier semaphores. Data moves between devices by JAX's collectives and lax.ppermute only.
A program may use at most 64 MiB of HBM per device.

```python
import math
import jax
import jax.numpy as jnp
import numpy as np
from jax import lax

D = 2048
HIDDEN_SIZE = 384
ROWS = 128
TOK_DEV = 128
EXPERTS = 8
CAP = 24
N_EP = 8
N_DP = 4


def draw_row_counts(key, part):
    first_key, second_key, third_key = jax.random.split(jax.random.fold_in(key, 17), 3)
    live_total = jax.random.randint(first_key, (N_DP, N_EP), ROWS // 2, ROWS + 1)
    fullest = jax.random.randint(second_key, (N_DP,), 0, N_EP)
    live_total = jnp.where(jnp.arange(N_EP)[None, :] == fullest[:, None], ROWS, live_total)
    home_share = jax.random.randint(third_key, (N_DP, N_EP), 0, live_total + 1)
    return jnp.stack([home_share, live_total - home_share], -1).astype(jnp.int32)


def plant(array, key, least, top_value):
    extent = array.shape
    index_at = [jax.random.randint(jax.random.fold_in(key, axis), (), 0, extent[axis]) for axis in range(len(extent))]
    array = array.at[tuple(index_at)].set(least)
    longest = extent.index(max(extent))
    index_at[longest] = (index_at[longest] + 1) % extent[longest]
    return array.at[tuple(index_at)].set(top_value)


def block_scale(key, shape, shards, smallest, high):
    loudness = 1.0
    for dim, shards_of in shards:
        draws = jax.random.uniform(jax.random.fold_in(jax.random.fold_in(key, 6), dim), (shards_of,), jnp.float32, smallest / len(shards), high / len(shards))
        loudness = loudness * jnp.repeat(jnp.exp(draws), shape[dim] // shards_of).reshape((-1,) + (1,) * (len(shape) - 1 - dim))
    return loudness


def routed_block(key, own, number, rows, number_of, top, bound, slope):
    ranking = jax.random.permutation(key, number_of)
    crowded, common = portions_of(number_of, rows * top, bound, slope, True), portions_of(number_of, rows * top, bound, slope, False)
    places = jnp.arange(number_of)

    def named(sizes, turn):
        used = int((sizes > 0).sum())
        fixed = max(1, used // 4)
        moved = fixed + (places - fixed + turn * (used - fixed)) % max(1, number_of - fixed)
        return jnp.zeros((number_of,), jnp.int32).at[ranking[jnp.where(places < fixed, places, moved)]].set(jnp.asarray(sizes, jnp.int32))

    sizes = jnp.where(number % 4 == 0, named(crowded, number // 4), named(common, number - number // 4 - 1))
    mixed = jax.random.permutation(jax.random.fold_in(own, 3), number_of)
    source_of, sink = mixed[0:number_of // 2 * 2:2], mixed[1:number_of // 2 * 2:2]
    room = jnp.minimum(sizes[source_of] - 1, bound - sizes[sink]) // 2
    room = jnp.where((source_of == ranking[0]) | (sink == ranking[0]) | (sizes[sink] == 0), 0, jnp.maximum(room, 0))
    moved = jax.random.randint(jax.random.fold_in(own, 4), (number_of // 2,), 0, 1 << 20) % (room + 1)
    sizes = sizes.at[source_of].add(-moved).at[sink].add(moved)
    labels = jnp.searchsorted(jnp.cumsum(sizes), jnp.arange(rows * top), side="right").astype(jnp.int32)
    table = labels.reshape(top, rows).T
    table = table[jax.random.permutation(jax.random.fold_in(own, 1), rows)]
    turn = jax.random.randint(jax.random.fold_in(own, 2), (rows, 1), 0, top)
    return jnp.take_along_axis(table, (jnp.arange(top)[None, :] + turn) % top, axis=1)


def portions_of(count, total, bound, skew, full):
    portions = [(1 << 20) // math.isqrt(standing ** skew) + 1 for standing in range(1, count + 1)]
    largest = bound if full else min(bound, max(-(-total // count), total * portions[0] // sum(portions)))
    least = 1 if total - largest >= count - 1 else 0
    given, rest = [largest] + [least] * (count - 1), total - largest - least * (count - 1)
    while rest > 0:
        candidates = [i for i in range(1, count) if given[i] < largest] or [i for i in range(1, count) if given[i] < bound]
        mass, remaining = sum([portions[i] for i in candidates]), rest
        for i in candidates:
            addition = min(bound - given[i], max(1, remaining * portions[i] // mass), rest)
            given[i] = given[i] + addition
            rest = rest - addition
    return np.array(given)


def gaussian(stream_key, shape, spread, limit, pieces=(), kind=jnp.bfloat16):
    gain = block_scale(stream_key, shape, pieces, -0.22, 0.18) if pieces else 1.0
    array = jax.random.normal(stream_key, shape, jnp.float32) * spread * gain
    return jnp.minimum(jnp.maximum(array, -limit), limit).astype(kind)


def setup_inputs(seed: int = 0) -> dict:
    arg_keys = jax.random.split(jax.random.key(seed), 9)
    row_inputs = gaussian(arg_keys[0], (N_DP, N_EP * ROWS, D), 1.0, 6.0, ((0, 4), (1, 8)))
    hidden_grad = gaussian(arg_keys[1], (N_DP, N_EP * ROWS, HIDDEN_SIZE), 1.0, 6.0, ((0, 4), (1, 8)))
    router_weight = jnp.clip(jnp.exp(math.log(1.0) - 2.9996462 * jax.random.uniform(arg_keys[2], (N_DP, N_EP * ROWS), jnp.float32) ** block_scale(arg_keys[2], (N_DP, N_EP * ROWS), ((0, 4), (1, 8)), -0.2, 0.2)), 0.049804688, 1.0).astype(jnp.bfloat16)
    row_counts = draw_row_counts(jax.random.fold_in(arg_keys[8], 71), 0)
    row_owner_keys = jax.random.split(jax.random.fold_in(arg_keys[4], 1), N_DP * (N_EP * ROWS) // ROWS)
    row_owner_turns = jax.random.permutation(jax.random.fold_in(arg_keys[4], 3), N_DP * (N_EP * ROWS) // ROWS)
    row_owner = jax.vmap(lambda own, number: routed_block(jax.random.fold_in(arg_keys[4], 2), own, number, ROWS, N_EP, 1, CAP, 1))(row_owner_keys, row_owner_turns).reshape((N_DP, N_EP * ROWS, 1))
    row_position = plant(jax.random.randint(arg_keys[5], (N_DP, N_EP * ROWS), 0, TOK_DEV), jax.random.fold_in(arg_keys[5], 1), 0, TOK_DEV - 1).astype(jnp.int32)
    replica_expert = jax.random.permutation(arg_keys[6], EXPERTS).astype(jnp.int32)
    gate_up = gaussian(arg_keys[7], (EXPERTS, D, 2 * HIDDEN_SIZE), D ** -0.5, 0.125, ((0, 8), (1, 4)))
    return dict(row_inputs=row_inputs, hidden_grad=hidden_grad, router_weight=router_weight, row_counts=row_counts, row_owner=row_owner, row_position=row_position, replica_expert=replica_expert, gate_up=gate_up)


def slot_terms(own_rows, own_grads, own_probs, live_rows, weights):
    pre = jnp.dot(own_rows, weights, preferred_element_type=jnp.float32)
    gate_pre = pre[:, :HIDDEN_SIZE]
    up_pre = pre[:, HIDDEN_SIZE:]
    sigmoid_gate = jax.nn.sigmoid(gate_pre)
    act_grad = jnp.where(live_rows[:, None], own_probs.astype(jnp.float32)[:, None] * own_grads.astype(jnp.float32), jnp.float32(0.0))
    up_grad = act_grad * gate_pre * sigmoid_gate
    gate_grad = act_grad * up_pre * sigmoid_gate * (1.0 + gate_pre * (1.0 - sigmoid_gate))
    pre_grad = jnp.concatenate([gate_grad, up_grad], 1).astype(jnp.bfloat16)
    row_grad = lax.dot_general(pre_grad, weights, (((1,), (1,)), ((), ())), preferred_element_type=jnp.float32)
    weight_part = lax.dot_general(own_rows, pre_grad, (((0,), (0,)), ((), ())), preferred_element_type=jnp.float32)
    return row_grad, weight_part.astype(jnp.bfloat16)


def reference(row_inputs, hidden_grad, router_weight, row_counts, row_owner, row_position, replica_expert, gate_up):
    positions = jnp.arange(ROWS, dtype=jnp.int32)
    inverse = jnp.zeros((N_EP,), jnp.int32).at[replica_expert].set(jnp.arange(N_EP, dtype=jnp.int32))
    row_blocks = row_inputs.reshape(N_DP, N_EP, ROWS, D)
    grad_blocks = hidden_grad.reshape(N_DP, N_EP, ROWS, HIDDEN_SIZE)
    prob_blocks = router_weight.reshape(N_DP, N_EP, ROWS)
    home_count = row_counts[:, :, 0:1]
    home_live = positions[None, None, :] < home_count
    rep_live = (positions[None, None, :] >= home_count) & (positions[None, None, :] < home_count + row_counts[:, :, 1:2])

    def per_expert(expert):
        weights = gate_up[expert]
        source = inverse[expert]

        def per_data(data_index):
            home_dx, home_part = slot_terms(row_blocks[data_index, expert], grad_blocks[data_index, expert], prob_blocks[data_index, expert], home_live[data_index, expert], weights)
            rep_dx, rep_part = slot_terms(row_blocks[data_index, source], grad_blocks[data_index, source], prob_blocks[data_index, source], rep_live[data_index, source], weights)
            home_wide = lax.optimization_barrier(home_part).astype(jnp.float32)
            rep_wide = lax.optimization_barrier(rep_part).astype(jnp.float32)
            summed = lax.optimization_barrier((home_wide + rep_wide).astype(jnp.bfloat16)).astype(jnp.float32)
            return home_dx.astype(jnp.bfloat16), rep_dx.astype(jnp.bfloat16), summed

        home_dx, rep_dx, summed = lax.map(per_data, jnp.arange(N_DP, dtype=jnp.int32))
        return home_dx, rep_dx, jnp.sum(summed, 0)

    home_dx, rep_dx, weight_grad = lax.map(per_expert, jnp.arange(EXPERTS, dtype=jnp.int32))
    row_dx = home_dx.astype(jnp.float32) + rep_dx[replica_expert].astype(jnp.float32)
    row_dx = jnp.transpose(row_dx, (1, 0, 2, 3)).reshape(N_DP, N_EP * ROWS, D)
    target = row_owner[:, :, 0] * TOK_DEV + row_position

    def gather_tokens(data_rows, data_ids):
        return jax.ops.segment_sum(data_rows, data_ids, num_segments=N_EP * TOK_DEV)

    token_grad = jax.vmap(gather_tokens)(row_dx, target).astype(jnp.bfloat16)
    return token_grad, weight_grad
```

```python
import functools

import jax
import jax.numpy as jnp
from jax import lax
from jax.experimental import pallas as pl
from jax.experimental.pallas import tpu as pltpu
from jax.sharding import PartitionSpec as P

F32 = jnp.float32
BF16 = jnp.bfloat16
VMEM = pl.BlockSpec(memory_space=pltpu.VMEM)
SMEM = pl.BlockSpec(memory_space=pltpu.SMEM)


def dot(a, b, dims=((1,), (0,))):
    return lax.dot_general(a, b, (dims, ((), ())), preferred_element_type=F32)


def routing_kernel(ids, rep_row, meta, ctl, where_home, where_rep, *, cap):
    n, rows = meta.shape[0], meta.shape[1] // 2
    me, source = ids[0], ids[1]
    total = n * rows
    r0 = lax.broadcasted_iota(jnp.int32, (rows, rows), 0)
    r1 = lax.broadcasted_iota(jnp.int32, (rows, rows), 1)
    before = (r0 < r1).astype(BF16)

    def parts(code):
        rep = code >= total
        live_target = jnp.where(rep, code - total, code)
        owner = jnp.where(code < 0, -1, lax.div(jnp.maximum(live_target, 0), rows))
        return owner, live_target - owner * rows, (code >= 0) & ~rep, rep

    code = meta[:, :rows].astype(jnp.int32)
    owner, position, home, rep = parts(code)
    lanes = lax.broadcasted_iota(jnp.int32, where_home.shape, 1)

    def positions_of(mask):
        rank = dot(mask.astype(BF16), before).astype(jnp.int32)
        found = jnp.zeros(where_home.shape, jnp.int32)
        for slot in range(cap):
            hit = jnp.where(mask & (rank == slot), position + 1, 0)
            found = jnp.where(lanes == slot, jnp.sum(hit, 1, keepdims=True), found)
        return found

    mine = owner == me
    where_home[...] = positions_of(mine & home) - 1
    e0 = lax.broadcasted_iota(jnp.int32, (n, n), 0)
    to_expert = (rep_row[...] == e0).astype(BF16)
    by_block = positions_of(mine & rep).astype(F32).astype(BF16)
    where_rep[...] = dot(to_expert, by_block).astype(jnp.int32) - 1

    owners = lax.broadcasted_iota(jnp.int32, (n, rows), 0)
    for which, block in ((0, me), (1, source)):
        line = meta[pl.ds(block, 1), :]
        own, _, h, r = parts(line[:, :rows].astype(jnp.int32))
        live = r if which else h
        held = (owners == own) & live
        count = dot(held.astype(BF16), before)
        rank = jnp.sum(jnp.where(held, count, 0.0), 0, keepdims=True)
        slot = jnp.where(live, own.astype(F32) * cap + rank, -1.0)
        ctl[2 * which : 2 * which + 1, :] = slot
        ctl[2 * which + 1 : 2 * which + 2, :] = jnp.where(live, line[:, rows:], 0.0)


def expert_kernel(ids, data, ctl, *refs, which, pieces, width, hidden):
    weights, (send, grads) = refs[:pieces], refs[pieces:]
    d = ids[2]
    rows = data.shape[0]
    cols = [pl.ds(pl.multiple_of((d ^ m) * width, width), width) for m in range(pieces)]
    pre = dot(data[:, cols[0]], weights[0][...])
    for m in range(1, pieces):
        pre = pre + dot(data[:, cols[m]], weights[m][...])
    r0 = lax.broadcasted_iota(jnp.int32, (rows, rows), 0)
    r1 = lax.broadcasted_iota(jnp.int32, (rows, rows), 1)
    prob = jnp.sum(
        jnp.where(r0 == r1, ctl[2 * which + 1 : 2 * which + 2, :], 0.0), 1, keepdims=True
    )
    act_grad = prob * data[:, pieces * width :].astype(F32)
    gate, up = pre[:, :hidden], pre[:, hidden:]
    s = jax.nn.sigmoid(gate)
    gate_grad = act_grad * up * s * (1.0 + gate * (1.0 - s))
    up_grad = act_grad * gate * s
    pre_grad = jnp.concatenate([gate_grad, up_grad], 1).astype(BF16)
    grads[...] = pre_grad
    slots = lax.broadcasted_iota(jnp.int32, (send.shape[0], rows), 0)
    place = (slots == ctl[2 * which : 2 * which + 1, :].astype(jnp.int32)).astype(BF16)
    placed = dot(place, pre_grad).astype(BF16)
    for m in range(pieces):
        send[:, cols[m]] = dot(placed, weights[m][...], ((1,), (1,))).astype(BF16)


def weight_kernel(ids, home_data, rep_data, home_grads, rep_grads, keep, give, *, pieces, width):
    d = ids[2]
    grads = jnp.concatenate([home_grads[...], rep_grads[...]], 0)
    for m in range(pieces):
        cols = pl.ds(pl.multiple_of((d ^ m) * width, width), width)
        data = jnp.concatenate([home_data[:, cols], rep_data[:, cols]], 0)
        part = dot(data, grads, ((0,), (0,))).astype(BF16)
        (give if m & 1 else keep)[m >> 1] = part


def body(row_inputs, hidden_grad, router_weight, row_counts, row_owner, row_position, replica_expert, gate_up):
    n, nd = lax.axis_size("ep"), lax.axis_size("dp")
    me, d = lax.axis_index("ep"), lax.axis_index("dp")
    rows, model = row_inputs.shape[1:]
    hidden = hidden_grad.shape[2]
    width = gate_up.shape[1]
    cap = max(2, 3 * rows // (2 * n))
    params = pltpu.CompilerParams(vmem_limit_bytes=48 << 20)

    def swap(array, bit):
        return lax.ppermute(array, "dp", [(i, i ^ bit) for i in range(nd)])

    def exchange(array):
        return lax.all_to_all(array, "ep", split_axis=0, concat_axis=0, tiled=True)

    own = gate_up[0]
    pieces = {0: own}
    bit = nd >> 1
    while bit:
        for m in list(pieces):
            pieces[m | bit] = swap(pieces[m], bit)
        bit >>= 1
    weights = [pieces[m] for m in range(nd)]

    payload = jnp.concatenate([row_inputs[0], hidden_grad[0]], 1)
    experts = jnp.arange(n, dtype=jnp.int32)
    inverse = jnp.sum(jnp.where(replica_expert[None, :] == experts[:, None], experts[None, :], 0), 1)
    spread = exchange(payload.reshape(n, rows // n, -1))
    routed = jnp.take(spread, inverse, axis=0, mode="clip")
    arrived = exchange(routed).reshape(rows, -1)

    at = jnp.arange(rows, dtype=jnp.int32)
    first, second = row_counts[0, 0, 0], row_counts[0, 0, 1]
    target = row_owner[0, :, 0] * rows + row_position[0]
    code = jnp.where(at < first, target, jnp.where(at < first + second, target + n * rows, -1))
    meta = jnp.concatenate([code.astype(F32), router_weight[0].astype(F32)])
    meta = exchange(jnp.broadcast_to(meta[None, None, :], (n, 1, 2 * rows))).reshape(n, 2 * rows)

    ids = jnp.stack([me, jnp.sum(jnp.where(experts == me, inverse, 0)), d]).astype(jnp.int32)
    ctl, where_home, where_rep = pl.pallas_call(
        functools.partial(routing_kernel, cap=cap),
        out_shape=(
            jax.ShapeDtypeStruct((8, rows), F32),
            jax.ShapeDtypeStruct((n, cap), jnp.int32),
            jax.ShapeDtypeStruct((n, cap), jnp.int32),
        ),
        in_specs=[SMEM, VMEM, VMEM],
        out_specs=(VMEM, VMEM, VMEM),
        name="routing",
    )(ids, replica_expert[None, :], meta)

    def expert(which, data):
        return pl.pallas_call(
            functools.partial(expert_kernel, which=which, pieces=nd, width=width, hidden=hidden),
            out_shape=(
                jax.ShapeDtypeStruct((n * cap, model), BF16),
                jax.ShapeDtypeStruct((rows, 2 * hidden), BF16),
            ),
            in_specs=[SMEM] + [VMEM] * (2 + nd),
            out_specs=(VMEM, VMEM),
            compiler_params=params,
            cost_estimate=pl.CostEstimate(flops=6 * rows * model * 2 * hidden, bytes_accessed=6 << 20, transcendentals=0),
            name=("home", "replica")[which],
        )(ids, data, ctl, *weights)

    tokens = jnp.arange(rows, dtype=jnp.int32)[:, None]

    def gathered(send, where_to):
        got = exchange(send.reshape(n, cap, model)).reshape(n * cap, model)
        pick = (where_to.reshape(1, -1) == tokens).astype(BF16)
        return jnp.dot(pick, got, preferred_element_type=F32)

    home_send, home_grads = expert(0, payload)
    home_tokens = gathered(home_send, where_home)
    rep_send, rep_grads = expert(1, arrived)
    token_grad = (home_tokens + gathered(rep_send, where_rep)).astype(BF16)

    keep, give = pl.pallas_call(
        functools.partial(weight_kernel, pieces=nd, width=width),
        out_shape=(jax.ShapeDtypeStruct((nd // 2, width, 2 * hidden), BF16),) * 2,
        in_specs=[SMEM] + [VMEM] * 4,
        out_specs=(VMEM, VMEM),
        compiler_params=params,
        cost_estimate=pl.CostEstimate(flops=8 * rows * model * hidden, bytes_accessed=6 << 20, transcendentals=0),
        name="weight_grad",
    )(ids, payload, arrived, home_grads, rep_grads)
    near = swap(give, 1)
    total = keep.astype(F32) + near.astype(F32)
    bit, held = nd >> 1, total
    while bit > 1:
        half = held.shape[0] // 2
        held = held[:half] + swap(held[half:].astype(BF16), bit).astype(F32)
        bit >>= 1
    return (token_grad[None], held)


def solution(mesh):
    placed = (
        P("dp", "ep", None),
        P("dp", "ep", None),
        P("dp", "ep"),
        P("dp", "ep", None),
        P("dp", "ep", None),
        P("dp", "ep"),
        P(),
        P("ep", "dp", None),
    )
    return jax.shard_map(
        body,
        mesh=mesh,
        in_specs=placed,
        out_specs=(P("dp", "ep", None), P("ep", "dp", None)),
        check_vma=False,
    )
```
